512 devices in a mesh: group: 64 (over y, z_hi, x, core), tensor: 8 (over z_lo).
Axes of the slice: x: 4, y: 4, z: 16 (z_hi: 2, z_lo: 8; z = z_hi * 8 + z_lo), core: 2. Of those that a mesh axis runs over, the one named last changes fastest.
Arguments:
- prompt_cache: bfloat16 [2, 262144, 1024], P(None, ('group', 'tensor')), may hold values from -6 to 6
- queries: bfloat16 [128, 64, 8192], P('group', None, 'tensor'), may hold values from -10 to 10
- new_cache: bfloat16 [2, 128, 64, 1024], P(None, 'group', None, 'tensor'), may hold values from -6 to 6
- offsets: int32 [64, 2], P('group'), may hold values from 0 to 3
- lengths: int32 [64], P('group'), may hold values from 64 to 4096
- block_table: int32 [64, 32], P('group'), may hold values from 0 to 31, each once within a row
Outputs:
- attention: bfloat16 [128, 64, 8192], P('group', None, 'tensor')
The draws below stay inside these ranges and needn't reach their ends.
Inputs may be any that keep to these rules, and one draw needn't show every extreme that they name: Each row of block_table names each of the 32 stored blocks of its prompt once.
All inputs are finite; a program needn't handle non-finite values.
Results may differ from the reference program's by a relative error of at most 0.0095.
Values may be sent and summed in bfloat16 or wider, within the bound.
No kernel may reach another device: no remote copies, remote signals or barrier semaphores. Data moves between devices by JAX's collectives and lax.ppermute only.
A program may use at most 64 MiB of HBM per device.

```python
import jax
import jax.numpy as jnp
from jax import lax

QH = 64
KVH = 8
HD = 128
BLOCK = 128
MAXB = 32
SAMPLES = 16
STEPS = 4
REACH = 4
CAP = 2
N_GROUP = 64


def base_queries(key):
    array_shape = (N_GROUP * CAP, SAMPLES * STEPS, QH * HD)
    drawn = jax.random.normal(jax.random.fold_in(key, 2101), array_shape, jnp.float32)
    return jnp.clip(drawn, -6.0, 6.0)


def draw_queries(key, part):
    drawn = base_queries(key)
    return drawn.astype(jnp.bfloat16)


def draw_prompt_cache(key, part):
    tokens = N_GROUP * MAXB * BLOCK
    array_shape = (2, tokens, KVH * HD)
    drawn = jnp.clip(jax.random.normal(jax.random.fold_in(key, 1101), array_shape, jnp.float32), -6.0, 6.0)
    return drawn.astype(jnp.bfloat16)


def draw_new_cache(key, part):
    array_shape = (N_GROUP * CAP, SAMPLES * STEPS, KVH * HD)
    grouped = base_queries(key).reshape(N_GROUP * CAP, SAMPLES * STEPS, KVH, QH // KVH, HD)
    grouped = jnp.mean(grouped, axis=3).reshape(array_shape)
    noise = jax.random.normal(jax.random.fold_in(key, 3101), array_shape, jnp.float32)
    key_part = jnp.clip(3.5 * grouped + 0.5 * noise, -6.0, 6.0)
    values = jnp.clip(jax.random.normal(jax.random.fold_in(key, 3102), array_shape, jnp.float32), -6.0, 6.0)
    return jnp.stack([key_part, values]).astype(jnp.bfloat16)


def place_ends(result, own_key, smallest, top_value):
    dims = result.shape
    place = [jax.random.randint(jax.random.fold_in(own_key, axis), (), 0, dims[axis]) for axis in range(len(dims))]
    result = result.at[tuple(place)].set(smallest)
    longest = dims.index(max(dims))
    place[longest] = (place[longest] + 1) % dims[longest]
    return result.at[tuple(place)].set(top_value)


def setup_inputs(seed: int = 0) -> dict:
    splits = jax.random.split(jax.random.key(seed), 7)
    prompt_cache = draw_prompt_cache(jax.random.fold_in(splits[6], 71), 0)
    queries = draw_queries(jax.random.fold_in(splits[6], 71), 0)
    new_cache = draw_new_cache(jax.random.fold_in(splits[6], 71), 0)
    offsets = place_ends(jax.random.randint(splits[3], (N_GROUP, CAP), 0, REACH), jax.random.fold_in(splits[3], 1), 0, REACH - 1).astype(jnp.int32)
    lengths = place_ends(jax.random.randint(splits[4], (N_GROUP,), BLOCK // 2, MAXB * BLOCK + 1), jax.random.fold_in(splits[4], 1), BLOCK // 2, MAXB * BLOCK).astype(jnp.int32)
    block_table = jax.vmap(lambda own: jax.random.permutation(own, MAXB))(jax.random.split(splits[5], N_GROUP)).reshape((N_GROUP, MAXB)).astype(jnp.int32)
    return {"prompt_cache": prompt_cache, "queries": queries, "new_cache": new_cache, "offsets": offsets, "lengths": lengths, "block_table": block_table}


masked_score = -1e30


def live_tokens(table_row, length, block_size):
    blocks = table_row.shape[0]
    physical = jnp.arange(blocks, dtype=jnp.int32)
    logical = jnp.sum(physical[:, None] * (table_row[:, None] == physical[None, :]).astype(jnp.int32), axis=0)
    position = logical[:, None] * block_size + jnp.arange(block_size, dtype=jnp.int32)[None, :]
    return position.reshape(-1) < length


def prompt_block(query_rows, prompt_keys, prompt_values, live_mask):
    row_count = query_rows.shape[0]
    kv_heads = prompt_keys.shape[1] // HD
    group_size = query_rows.shape[1] // (kv_heads * HD)
    query_split = query_rows.astype(jnp.float32).reshape(row_count, kv_heads, group_size, HD)
    key_split = prompt_keys.astype(jnp.float32).reshape(-1, kv_heads, HD)
    value_split = prompt_values.astype(jnp.float32).reshape(-1, kv_heads, HD)
    scores = jnp.einsum("rgkd,pgd->gkrp", query_split, key_split, precision=lax.Precision.HIGHEST) * (HD ** -0.5)
    scores = jnp.where(live_mask[None, None, None, :], scores, masked_score)
    prompt_peak = jnp.max(scores, axis=-1)
    weights = jnp.exp(scores - prompt_peak[..., None])
    prompt_total = jnp.sum(weights, axis=-1)
    rounded = lax.optimization_barrier(weights.astype(jnp.bfloat16)).astype(jnp.float32)
    numerator = jnp.einsum("gkrp,pgd->rgkd", rounded, value_split, precision=lax.Precision.HIGHEST)
    total_rows = jnp.transpose(prompt_total, (2, 0, 1))
    prompt_part = (numerator / total_rows[..., None]).astype(jnp.bfloat16)
    return prompt_part, jnp.transpose(prompt_peak, (2, 0, 1)), total_rows


def own_block(query_rows, new_keys, new_values):
    kv_heads = new_keys.shape[1] // HD
    group_size = query_rows.shape[1] // (kv_heads * HD)
    row_count = SAMPLES * STEPS
    query_split = query_rows.astype(jnp.float32).reshape(SAMPLES, STEPS, kv_heads, group_size, HD)
    key_split = new_keys.astype(jnp.float32).reshape(SAMPLES, STEPS, kv_heads, HD)
    value_split = new_values.astype(jnp.float32).reshape(SAMPLES, STEPS, kv_heads, HD)
    scores = jnp.einsum("stgkd,sugd->stgku", query_split, key_split, precision=lax.Precision.HIGHEST) * (HD ** -0.5)
    steps_index = jnp.arange(STEPS, dtype=jnp.int32)
    causal = (steps_index[:, None] >= steps_index[None, :])[None, :, None, None, :]
    scores = jnp.where(causal, scores, masked_score)
    own_peak = jnp.max(scores, axis=-1)
    weights = jnp.exp(scores - own_peak[..., None])
    own_total = jnp.sum(weights, axis=-1)
    rounded = lax.optimization_barrier(weights.astype(jnp.bfloat16)).astype(jnp.float32)
    own_sum = jnp.einsum("stgku,sugd->stgkd", rounded, value_split, precision=lax.Precision.HIGHEST)
    return (own_sum.reshape(row_count, kv_heads, group_size, HD),
            own_peak.reshape(row_count, kv_heads, group_size),
            own_total.reshape(row_count, kv_heads, group_size))


def merge_parts(prompt_stats, own_stats):
    prompt_part, prompt_peak, prompt_total = prompt_stats
    own_sum, own_peak, own_total = own_stats
    prompt_part = lax.optimization_barrier(prompt_part)
    highest = jnp.maximum(prompt_peak, own_peak)
    prompt_scale = prompt_total * jnp.exp(prompt_peak - highest)
    own_scale = jnp.exp(own_peak - highest)
    numerator_all = prompt_scale[..., None] * prompt_part.astype(jnp.float32) + own_scale[..., None] * own_sum
    denominator = prompt_scale + own_total * own_scale
    merged = numerator_all / denominator[..., None]
    return merged.reshape(merged.shape[0], -1).astype(jnp.bfloat16)


def reference(prompt_cache, queries, new_cache, offsets, lengths, block_table):
    prompt_tokens = MAXB * BLOCK
    all_keys = prompt_cache[0]
    all_values = prompt_cache[1]
    new_keys_all = new_cache[0]
    new_values_all = new_cache[1]
    flat_offsets = offsets.reshape(-1)

    def serve_slot(slot):
        decode_group = slot // CAP
        distance = flat_offsets[slot]
        prompt = ((decode_group - distance) % N_GROUP).astype(jnp.int32)
        start = (prompt * prompt_tokens).astype(jnp.int32)
        prompt_keys = lax.dynamic_slice_in_dim(all_keys, start, prompt_tokens, 0)
        prompt_values = lax.dynamic_slice_in_dim(all_values, start, prompt_tokens, 0)
        live_mask = live_tokens(block_table[prompt], lengths[prompt], BLOCK)
        query_rows = lax.dynamic_index_in_dim(queries, slot, 0, keepdims=False)
        new_keys = lax.dynamic_index_in_dim(new_keys_all, slot, 0, keepdims=False)
        new_values = lax.dynamic_index_in_dim(new_values_all, slot, 0, keepdims=False)
        prompt_stats = prompt_block(query_rows, prompt_keys, prompt_values, live_mask)
        own_stats = own_block(query_rows, new_keys, new_values)
        return merge_parts(prompt_stats, own_stats)

    indices = jnp.arange(N_GROUP * CAP, dtype=jnp.int32)
    return lax.map(serve_slot, indices)
```

```python
from functools import partial

import jax
import jax.numpy as jnp
from jax import lax
from jax.experimental import pallas as pl
from jax.experimental.pallas import tpu as pltpu
from jax.sharding import PartitionSpec as P


HD = 128
BLOCK = 128
STEPS = 4
REACH = 4
ROW = 8
TAG = 16
PART = 4
HEADS = 8
QROWS = 64
MSG = HEADS * HD + 128
MASKED = -1e30
ORDER = ((0, 4, 1, 5), (2, 6, 3), (7,))
SCALE2 = 1.4426950408889634 * HD ** (-0.5)


def head_rows(q):
    return jnp.concatenate([q[:, h * HD:(h + 1) * HD] for h in range(HEADS)], axis=0)


def scores_of(q, k):
    return lax.dot_general(q, k, (((1,), (1,)), ((), ())), preferred_element_type=jnp.float32) * SCALE2


def split3(x):
    hi = x.astype(jnp.bfloat16).astype(jnp.float32)
    rest = x - hi
    mid = rest.astype(jnp.bfloat16).astype(jnp.float32)
    return hi, mid, rest - mid


def flash_kernel(n_chunks, lo, first, outs_of, wanted_ref, bias_ref, q_ref, *refs):
    k_wide, v_wide = refs[-2:]
    kv_refs = refs[:n_chunks]
    refs = refs[n_chunks:-2]
    if first:
        outs = refs
    else:
        acc_in, top_in = refs[:2]
        outs = refs[2:]
    tokens = kv_refs[0].shape[1]
    step = pl.program_id(0)

    @pl.when(step == 0)
    def _():
        for m in range(n_chunks):
            rows = slice(m * tokens, (m + 1) * tokens)
            k_wide[rows, :HD] = kv_refs[m][0]
            v_wide[rows, :HD] = kv_refs[m][1]
        k_wide[:, HD:] = bias_ref[...]
        v_wide[:, HD:] = jnp.ones((n_chunks * tokens, HD), jnp.bfloat16)

    @pl.when(wanted_ref[lo + step] == 1)
    def _():
        lane = lax.broadcasted_iota(jnp.int32, (1, HD), 1)
        count = PART * QROWS
        mark = jnp.broadcast_to(jnp.where(lane == 0, 1.0, 0.0).astype(jnp.bfloat16), (count, HD))
        parts = []
        stats = jnp.zeros((QROWS, HD), jnp.float32)
        for block in range(HEADS // PART):
            rows = slice(block * count, (block + 1) * count)
            heads = range(block * PART, (block + 1) * PART)
            q = jnp.concatenate([q_ref[0, :, h * HD:(h + 1) * HD] for h in heads], axis=0)
            s = lax.dot_general(
                jnp.concatenate([q, mark], axis=1),
                k_wide[...],
                (((1,), (1,)), ((), ())),
                preferred_element_type=jnp.float32,
            )
            top = jnp.broadcast_to(jnp.max(s, axis=1, keepdims=True), (count, HD))
            if not first:
                old = top_in[0, rows]
                top = jnp.maximum(old, top)
            p = jnp.exp2((s - top[:, 0:1]) * SCALE2).astype(jnp.bfloat16)
            acc = jnp.dot(p, v_wide[...], preferred_element_type=jnp.float32)
            if not first:
                alpha = jnp.exp2((old - top) * SCALE2)
                acc = acc + acc_in[0, rows] * jnp.concatenate([alpha, alpha], axis=1)
            if outs_of is None:
                outs[0][0, rows] = acc
                outs[1][0, rows] = top
                continue
            parts.append((acc[:, :HD] / acc[:, HD:]).astype(jnp.bfloat16))
            big = split3(top * SCALE2 + jnp.log2(acc[:, HD:]))
            for index, h in enumerate(heads):
                mine = slice(index * QROWS, (index + 1) * QROWS)
                for c in range(3):
                    stats = jnp.where(lane == 3 * h + c, big[c][mine], stats)
        if outs_of is None:
            return
        for index, msg in enumerate(outs):
            for slot in range(outs_of):

                @pl.when(step == index * outs_of + slot)
                def _():
                    there = slice(slot * QROWS, (slot + 1) * QROWS)
                    for h in range(HEADS):
                        mine = slice(h % PART * QROWS, (h % PART + 1) * QROWS)
                        msg[there, h * HD:(h + 1) * HD] = parts[h // PART][mine]
                    msg[there, HEADS * HD:] = stats.astype(jnp.bfloat16)


def flash_call(wanted, bias, q_all, chunks, state, slots, caps, last=False):
    first = state is None
    lo, count = slots
    rows = HEADS * QROWS
    n = len(chunks)
    tokens = n * chunks[0].shape[1]
    at = lambda s, w: (lo + s, 0, 0)
    in_specs = [
        pl.BlockSpec(bias.shape, lambda s, w: (0, 0)),
        pl.BlockSpec((1, QROWS, HEADS * HD), lambda s, w: ((lo + s) // caps, (lo + s) % caps, 0)),
    ]
    in_specs += [pl.BlockSpec(c.shape, lambda s, w: (0, 0, 0)) for c in chunks]
    operands = [bias, q_all, *chunks]
    state_specs = [pl.BlockSpec((1, rows, 2 * HD), at), pl.BlockSpec((1, rows, HD), at)]
    if not first:
        in_specs += state_specs
        operands += list(state)
    if not last:
        out_specs = state_specs
        shapes = [(count, rows, 2 * HD), (count, rows, HD)]
        out_shape = [jax.ShapeDtypeStruct(s, jnp.float32) for s in shapes]
    else:
        out_specs = [pl.BlockSpec((caps * QROWS, MSG), lambda s, w: (0, 0))] * (count // caps)
        out_shape = [jax.ShapeDtypeStruct((caps * QROWS, MSG), jnp.bfloat16)] * (count // caps)
    return pl.pallas_call(
        partial(flash_kernel, n, lo, first, caps if last else None),
        grid_spec=pltpu.PrefetchScalarGridSpec(
            num_scalar_prefetch=1,
            grid=(count,),
            in_specs=in_specs,
            out_specs=out_specs,
            scratch_shapes=[pltpu.VMEM((tokens, 2 * HD), jnp.bfloat16)] * 2,
        ),
        out_shape=out_shape,
        compiler_params=pltpu.CompilerParams(dimension_semantics=("arbitrary",)),
        cost_estimate=pl.CostEstimate(
            flops=8 * count * rows * tokens * HD,
            transcendentals=count * rows * tokens,
            bytes_accessed=4 * tokens * HD,
        ),
        name="flash_last" if last else "flash_part",
    )(wanted, *operands)


def own_kernel(q_ref, new_ref, part_ref, stat_ref):
    lane = lax.broadcasted_iota(jnp.int32, (1, HD), 1)
    shape = (HEADS * QROWS, QROWS)
    query = lax.broadcasted_iota(jnp.int32, shape, 0) % QROWS
    token = lax.broadcasted_iota(jnp.int32, shape, 1)
    seen = (query // STEPS == token // STEPS) & (token <= query)
    for slot in range(q_ref.shape[0]):
        q = head_rows(q_ref[slot])
        s = jnp.where(seen, scores_of(q, new_ref[0, slot]), MASKED)
        m = jnp.max(s, axis=1, keepdims=True)
        p = jnp.exp2(s - m)
        l = jnp.sum(p, axis=1, keepdims=True)
        acc = jnp.dot(p.astype(jnp.bfloat16), new_ref[1, slot], preferred_element_type=jnp.float32)
        part = acc / l
        big = m + jnp.log2(l)
        stats = jnp.zeros((QROWS, HD), jnp.float32)
        for h in range(HEADS):
            rows = slice(h * QROWS, (h + 1) * QROWS)
            part_ref[slot, :, h * HD:(h + 1) * HD] = part[rows]
            stats = jnp.where(lane == h, big[rows], stats)
        stat_ref[slot] = stats


def own_call(queries, new_cache):
    slots = queries.shape[0]
    return pl.pallas_call(
        own_kernel,
        out_shape=[
            jax.ShapeDtypeStruct(queries.shape, jnp.float32),
            jax.ShapeDtypeStruct((slots, QROWS, HD), jnp.float32),
        ],
        name="own_part",
    )(queries, new_cache)


def merge_kernel(code_ref, m0, m1, m2, m3, m4, part_ref, stat_ref, out_ref, msg, sem):
    slots = out_ref.shape[0]
    for slot in range(slots):
        rows = pl.ds(slot * QROWS, QROWS)
        for index, ref in enumerate((m0, m1, m2, m3, m4)):

            @pl.when(code_ref[slot] == index)
            def _():
                pltpu.make_async_copy(ref.at[rows, :], msg.at[slot], sem.at[slot]).start()

    for slot in range(slots):
        rows = pl.ds(slot * QROWS, QROWS)
        pltpu.make_async_copy(m0.at[rows, :], msg.at[slot], sem.at[slot]).wait()
        stats = msg[slot, :, HEADS * HD:].astype(jnp.float32)
        own_stats = stat_ref[slot]
        for h in range(HEADS):
            cols = slice(h * HD, (h + 1) * HD)
            far = stats[:, 3 * h:3 * h + 1] + (
                stats[:, 3 * h + 1:3 * h + 2] + stats[:, 3 * h + 2:3 * h + 3]
            )
            near = own_stats[:, h:h + 1]
            top = jnp.maximum(far, near)
            far = jnp.exp2(far - top)
            near = jnp.exp2(near - top)
            scale = 1.0 / (far + near)
            out = (far * scale) * msg[slot, :, cols].astype(jnp.float32) + (
                near * scale
            ) * part_ref[slot, :, cols]
            out_ref[slot, :, cols] = out.astype(out_ref.dtype)


def merge_call(code, messages, own, shape):
    vmem = pl.BlockSpec(memory_space=pltpu.VMEM)
    anywhere = pl.BlockSpec(memory_space=pl.ANY)
    return pl.pallas_call(
        merge_kernel,
        in_specs=[pl.BlockSpec(memory_space=pltpu.SMEM)] + [anywhere] * 5 + [vmem] * 2,
        out_specs=vmem,
        out_shape=jax.ShapeDtypeStruct(shape, jnp.bfloat16),
        scratch_shapes=[
            pltpu.VMEM((shape[0], QROWS, MSG), jnp.bfloat16),
            pltpu.SemaphoreType.DMA((shape[0],)),
        ],
        name="merge",
    )(code, *messages, *own)


def live_bias(table_row, length, member, members):
    blocks = table_row.shape[0]
    per = blocks // members
    chunk = member ^ jnp.arange(members, dtype=jnp.int32)
    physical = chunk[:, None] * per + jnp.arange(per, dtype=jnp.int32)[None, :]
    logical = jnp.sum(
        jnp.where(
            table_row[None, None, :] == physical[:, :, None],
            jnp.arange(blocks, dtype=jnp.int32)[None, None, :],
            0,
        ),
        axis=2,
    )
    position = logical[:, :, None] * BLOCK + jnp.arange(BLOCK, dtype=jnp.int32)
    bias = jnp.where(position < length, 0.0, MASKED).astype(jnp.bfloat16)
    return bias.reshape(members, -1)


def shards(prompt_cache, queries, new_cache, offsets, lengths, block_table):
    groups = lax.axis_size("group")
    members = lax.axis_size("tensor")
    member = lax.axis_index("tensor")
    place = lax.axis_index("group") % ROW
    n_rows = groups // ROW

    def in_row(value, pairs):
        whole = [(r * ROW + a, r * ROW + b) for r in range(n_rows) for a, b in pairs]
        return lax.ppermute(value, "group", whole)

    def cross_row(value, pairs, step):
        whole = [
            (r * ROW + a, (r + step) % n_rows * ROW + b) for r in range(n_rows) for a, b in pairs
        ]
        return lax.ppermute(value, "group", whole)

    caps = queries.shape[0]
    last_row = caps * QROWS
    marks = jnp.repeat(offsets[0].astype(jnp.bfloat16), TAG // caps)
    tagged = jnp.concatenate(
        [
            queries.reshape(last_row, HEADS * HD),
            jnp.broadcast_to(marks[:, None], (TAG, HEADS * HD)),
        ],
        axis=0,
    )
    over = cross_row(tagged, [(0, 0), (1, 1), (2, 2)], -1)
    near = [in_row(tagged, [(i, i - k) for i in range(k, ROW)]) for k in range(1, REACH)]

    def slab(j):
        return lax.dynamic_slice_in_dim(prompt_cache, (member ^ j) * HD, HD, 2)

    def exchanged(j):
        value = slab(j)
        return lax.ppermute(value, "tensor", [(m, m ^ j) for m in range(members)])

    chunk = {j: exchanged(j) for j in range(1, members)}
    chunk[0] = slab(0)
    far = [in_row(over, [(i, ROW - k + i) for i in range(k)]) for k in range(1, REACH)]

    live = live_bias(block_table[0], lengths[0], member, members)
    biases = [
        jnp.broadcast_to(
            jnp.concatenate([live[j] for j in order])[:, None], (len(order) * live.shape[1], HD)
        )
        for order in ORDER
    ]
    q_all = jnp.stack(
        [tagged]
        + [jnp.where(place + k >= ROW, far[k - 1], near[k - 1]) for k in range(1, REACH)]
    )
    slots = REACH * caps
    asked = q_all[:, last_row::TAG // caps, 0].astype(jnp.int32)
    wanted = (asked == jnp.arange(REACH, dtype=jnp.int32)[:, None]).astype(jnp.int32).reshape(-1)
    code = jnp.where(place == 2, 3, jnp.where(asked[3] == 3, 0, asked[3]))
    pick = jnp.broadcast_to(jnp.repeat(code, QROWS)[:, None], (last_row, HD))
    source = jnp.where(offsets[0] <= place, offsets[0], REACH)
    own = own_call(queries, new_cache)
    q_all, wanted, own, pick, source, biases = lax.optimization_barrier(
        (q_all, wanted, own, pick, source, biases)
    )

    state = flash_call(wanted, biases[0], q_all, [chunk[j] for j in ORDER[0]], None, (0, slots), caps)
    state = flash_call(wanted, biases[1], q_all, [chunk[j] for j in ORDER[1]], state, (0, slots), caps)
    final = partial(flash_call, wanted, biases[2], q_all, [chunk[j] for j in ORDER[2]], state)
    message = [None, *final((caps, slots - caps), caps, True)]

    gathered = [
        in_row(message[1], [(7, 5)]),
        in_row(message[2], [(6, 5), (7, 6)]),
        in_row(message[3], [(7, 2)]),
    ]
    back = [in_row(message[k], [(i, i + k) for i in range(ROW - k)]) for k in range(1, REACH)]
    pick = pick[:, :1]
    passed = jnp.where(
        pick == 1,
        gathered[0],
        jnp.where(pick == 2, gathered[1], jnp.where(pick == 3, gathered[2], message[3])),
    )
    crossed = cross_row(passed, [(5, 0), (6, 1), (2, 2)], 1)
    (message[0],) = final((0, caps), caps, True)
    return merge_call(source, [message[0], *back, crossed], own, queries.shape)


def solution(mesh):
    in_specs = (
        P(None, ("group", "tensor"), None),
        P("group", None, "tensor"),
        P(None, "group", None, "tensor"),
        P("group", None),
        P("group"),
        P("group", None),
    )
    out_specs = P("group", None, "tensor")

    return jax.shard_map(shards, mesh=mesh, in_specs=in_specs, out_specs=out_specs, check_vma=False)
```

```python
from functools import partial

import jax
import jax.numpy as jnp
from jax import lax
from jax.experimental import pallas as pl
from jax.experimental.pallas import tpu as pltpu
from jax.sharding import PartitionSpec as P


HD = 128
BLOCK = 128
STEPS = 4
REACH = 4
ROW = 8
PART = 4
HEADS = 8
QROWS = 64
MSG = HEADS * HD + 128
MASKED = -1e30
ORDER = ((0, 1, 2, 3), (4, 5, 6), (7,))
SCALE2 = 1.4426950408889634 * HD ** (-0.5)


def head_rows(q):
    return jnp.concatenate([q[:, h * HD:(h + 1) * HD] for h in range(HEADS)], axis=0)


def scores_of(q, k):
    return lax.dot_general(q, k, (((1,), (1,)), ((), ())), preferred_element_type=jnp.float32) * SCALE2


def split3(x):
    hi = x.astype(jnp.bfloat16).astype(jnp.float32)
    rest = x - hi
    mid = rest.astype(jnp.bfloat16).astype(jnp.float32)
    return hi, mid, rest - mid


def flash_kernel(n_chunks, lo, first, outs_of, wanted_ref, bias_ref, q_ref, *refs):
    k_all, v_wide = refs[-2:]
    kv_refs = refs[:n_chunks]
    refs = refs[n_chunks:-2]
    if first:
        outs = refs
    else:
        acc_in, top_in = refs[:2]
        outs = refs[2:]
    tokens = kv_refs[0].shape[1]
    step = pl.program_id(0)

    @pl.when(step == 0)
    def _():
        for m in range(n_chunks):
            rows = slice(m * tokens, (m + 1) * tokens)
            k_all[rows, :] = kv_refs[m][0]
            v_wide[rows, :HD] = kv_refs[m][1]
        v_wide[:, HD:] = jnp.ones((n_chunks * tokens, HD), jnp.bfloat16)

    @pl.when(wanted_ref[lo + step] == 1)
    def _():
        lane = lax.broadcasted_iota(jnp.int32, (1, HD), 1)
        count = PART * QROWS
        parts = []
        stats = jnp.zeros((QROWS, HD), jnp.float32)
        for block in range(HEADS // PART):
            rows = slice(block * count, (block + 1) * count)
            heads = range(block * PART, (block + 1) * PART)
            q = jnp.concatenate([q_ref[0, :, h * HD:(h + 1) * HD] for h in heads], axis=0)
            s = lax.dot_general(
                q,
                k_all[...],
                (((1,), (1,)), ((), ())),
                preferred_element_type=jnp.float32,
            ) + bias_ref[...]
            top = jnp.broadcast_to(jnp.max(s, axis=1, keepdims=True), (count, HD))
            if not first:
                old = top_in[0, rows]
                top = jnp.maximum(old, top)
            p = jnp.exp2((s - top[:, 0:1]) * SCALE2).astype(jnp.bfloat16)
            acc = jnp.dot(p, v_wide[...], preferred_element_type=jnp.float32)
            if not first:
                alpha = jnp.exp2((old - top) * SCALE2)
                acc = acc + acc_in[0, rows] * jnp.concatenate([alpha, alpha], axis=1)
            if outs_of is None:
                outs[0][0, rows] = acc
                outs[1][0, rows] = top
                continue
            parts.append((acc[:, :HD] / acc[:, HD:]).astype(jnp.bfloat16))
            big = split3(top * SCALE2 + jnp.log2(acc[:, HD:]))
            for index, h in enumerate(heads):
                mine = slice(index * QROWS, (index + 1) * QROWS)
                for c in range(3):
                    stats = jnp.where(lane == c * HEADS + h, big[c][mine], stats)
        if outs_of is None:
            return
        for index, msg in enumerate(outs):
            for slot in range(outs_of):

                @pl.when(step == index * outs_of + slot)
                def _():
                    there = slice(slot * QROWS, (slot + 1) * QROWS)
                    for h in range(HEADS):
                        mine = slice(h % PART * QROWS, (h % PART + 1) * QROWS)
                        msg[there, h * HD:(h + 1) * HD] = parts[h // PART][mine]
                    msg[there, HEADS * HD:] = stats.astype(jnp.bfloat16)


def flash_call(wanted, bias, q_all, chunks, state, slots, caps, last=False):
    first = state is None
    lo, count = slots
    rows = HEADS * QROWS
    n = len(chunks)
    tokens = n * chunks[0].shape[1]
    at = lambda s, w: (lo + s, 0, 0)
    in_specs = [
        pl.BlockSpec(bias.shape, lambda s, w: (0, 0)),
        pl.BlockSpec((1, QROWS, HEADS * HD), lambda s, w: ((lo + s) // caps, (lo + s) % caps, 0)),
    ]
    in_specs += [pl.BlockSpec(c.shape, lambda s, w: (0, 0, 0)) for c in chunks]
    operands = [bias, q_all, *chunks]
    state_specs = [pl.BlockSpec((1, rows, 2 * HD), at), pl.BlockSpec((1, rows, HD), at)]
    if not first:
        in_specs += state_specs
        operands += list(state)
    if not last:
        out_specs = state_specs
        shapes = [(count, rows, 2 * HD), (count, rows, HD)]
        out_shape = [jax.ShapeDtypeStruct(s, jnp.float32) for s in shapes]
    else:
        out_specs = [pl.BlockSpec((caps * QROWS, MSG), lambda s, w: (0, 0))] * (count // caps)
        out_shape = [jax.ShapeDtypeStruct((caps * QROWS, MSG), jnp.bfloat16)] * (count // caps)
    return pl.pallas_call(
        partial(flash_kernel, n, lo, first, caps if last else None),
        grid_spec=pltpu.PrefetchScalarGridSpec(
            num_scalar_prefetch=1,
            grid=(count,),
            in_specs=in_specs,
            out_specs=out_specs,
            scratch_shapes=[
                pltpu.VMEM((tokens, HD), jnp.bfloat16),
                pltpu.VMEM((tokens, 2 * HD), jnp.bfloat16),
            ],
        ),
        out_shape=out_shape,
        compiler_params=pltpu.CompilerParams(dimension_semantics=("arbitrary",)),
        cost_estimate=pl.CostEstimate(
            flops=8 * count * rows * tokens * HD,
            transcendentals=count * rows * tokens,
            bytes_accessed=4 * tokens * HD,
        ),
        name="flash_last" if last else "flash_part",
    )(wanted, *operands)


def own_kernel(q_ref, new_ref, part_ref, stat_ref):
    lane = lax.broadcasted_iota(jnp.int32, (1, HD), 1)
    shape = (HEADS * QROWS, QROWS)
    query = lax.broadcasted_iota(jnp.int32, shape, 0) % QROWS
    token = lax.broadcasted_iota(jnp.int32, shape, 1)
    seen = (query // STEPS == token // STEPS) & (token <= query)
    for slot in range(q_ref.shape[0]):
        q = head_rows(q_ref[slot])
        s = jnp.where(seen, scores_of(q, new_ref[0, slot]), MASKED)
        m = jnp.max(s, axis=1, keepdims=True)
        p = jnp.exp2(s - m)
        l = jnp.sum(p, axis=1, keepdims=True)
        acc = jnp.dot(p.astype(jnp.bfloat16), new_ref[1, slot], preferred_element_type=jnp.float32)
        part = acc / l
        big = m + jnp.log2(l)
        stats = jnp.zeros((QROWS, HD), jnp.float32)
        for h in range(HEADS):
            rows = slice(h * QROWS, (h + 1) * QROWS)
            part_ref[slot, :, h * HD:(h + 1) * HD] = part[rows]
            stats = jnp.where(lane == h, big[rows], stats)
        stat_ref[slot] = stats


def own_call(queries, new_cache):
    slots = queries.shape[0]
    return pl.pallas_call(
        own_kernel,
        out_shape=[
            jax.ShapeDtypeStruct(queries.shape, jnp.float32),
            jax.ShapeDtypeStruct((slots, QROWS, HD), jnp.float32),
        ],
        name="own_part",
    )(queries, new_cache)


def merge_kernel(code_ref, m0, m1, m2, m3, m4, part_ref, stat_ref, out_ref, msg, sem):
    slots = out_ref.shape[0]
    for slot in range(slots):
        rows = pl.ds(slot * QROWS, QROWS)
        for index, ref in enumerate((m0, m1, m2, m3, m4)):

            @pl.when(code_ref[slot] == index)
            def _():
                pltpu.make_async_copy(ref.at[rows, :], msg.at[slot], sem.at[slot]).start()

    for slot in range(slots):
        rows = pl.ds(slot * QROWS, QROWS)
        pltpu.make_async_copy(m0.at[rows, :], msg.at[slot], sem.at[slot]).wait()
        stats = msg[slot, :, HEADS * HD:].astype(jnp.float32)
        far = stats + (
            pltpu.roll(stats, HD - HEADS, 1) + pltpu.roll(stats, HD - 2 * HEADS, 1)
        )
        near = stat_ref[slot]
        top = jnp.maximum(far, near)
        far = jnp.exp2(far - top)
        near = jnp.exp2(near - top)
        scale = 1.0 / (far + near)
        far = far * scale
        near = near * scale
        for h in range(HEADS):
            cols = slice(h * HD, (h + 1) * HD)
            out = far[:, h:h + 1] * msg[slot, :, cols].astype(jnp.float32) + (
                near[:, h:h + 1] * part_ref[slot, :, cols]
            )
            out_ref[slot, :, cols] = out.astype(out_ref.dtype)


def merge_call(code, messages, own, shape):
    vmem = pl.BlockSpec(memory_space=pltpu.VMEM)
    anywhere = pl.BlockSpec(memory_space=pltpu.HBM)
    return pl.pallas_call(
        merge_kernel,
        in_specs=[pl.BlockSpec(memory_space=pltpu.SMEM)] + [anywhere] * 5 + [vmem] * 2,
        out_specs=vmem,
        out_shape=jax.ShapeDtypeStruct(shape, jnp.bfloat16),
        scratch_shapes=[
            pltpu.VMEM((shape[0], QROWS, MSG), jnp.bfloat16),
            pltpu.SemaphoreType.DMA((shape[0],)),
        ],
        name="merge",
    )(code, *messages, *own)


def live_bias(table_row, length, member, members):
    blocks = table_row.shape[0]
    per = blocks // members
    chunk = member ^ jnp.arange(members, dtype=jnp.int32)
    physical = chunk[:, None] * per + jnp.arange(per, dtype=jnp.int32)[None, :]
    logical = jnp.sum(
        jnp.where(
            table_row[None, None, :] == physical[:, :, None],
            jnp.arange(blocks, dtype=jnp.int32)[None, None, :],
            0,
        ),
        axis=2,
    )
    position = logical[:, :, None] * BLOCK + jnp.arange(BLOCK, dtype=jnp.int32)
    bias = jnp.where(position < length, 0.0, MASKED).astype(jnp.float32)
    return bias.reshape(members, -1)


def shards(prompt_cache, queries, new_cache, offsets, lengths, block_table):
    groups = lax.axis_size("group")
    members = lax.axis_size("tensor")
    member = lax.axis_index("tensor")
    place = lax.axis_index("group") % ROW
    n_rows = groups // ROW

    def in_row(value, pairs):
        whole = [(r * ROW + a, r * ROW + b) for r in range(n_rows) for a, b in pairs]
        return lax.ppermute(value, "group", whole)

    def cross_row(value, pairs, step):
        whole = [
            (r * ROW + a, (r + step) % n_rows * ROW + b) for r in range(n_rows) for a, b in pairs
        ]
        return lax.ppermute(value, "group", whole)

    caps = queries.shape[0]
    last_row = caps * QROWS
    flat_q = queries.reshape(last_row, HEADS * HD)
    hop = in_row(flat_q, [(1, 5)])
    over = cross_row(jnp.where(place == 5, hop, flat_q), [(0, 0), (5, 5), (2, 2)], -1)
    inside = [[(i, i - k) for i in range(k, ROW)] for k in range(1, REACH)]
    tags = [in_row(offsets, inside[k - 1]) for k in range(1, REACH)]
    far_offsets = cross_row(offsets, [(0, 5), (1, 6)], -1)
    near = [in_row(flat_q, [(i, i - k) for i in range(k, ROW)]) for k in range(1, REACH)]

    def slab(j):
        return lax.dynamic_slice_in_dim(prompt_cache, (member ^ j) * HD, HD, 2)

    def exchanged(j):
        value = slab(j)
        return lax.ppermute(value, "tensor", [(m, m ^ j) for m in range(members)])

    chunk = {j: exchanged(j) for j in range(1, members)}
    chunk[0] = slab(0)
    far = [in_row(over, [((0, 5, 2)[i], ROW - k + i) for i in range(k)]) for k in range(1, REACH)]

    live = live_bias(block_table[0], lengths[0], member, members)
    biases = [jnp.concatenate([live[j] for j in order])[None, :] for order in ORDER]
    slots = REACH * caps
    outside = [place + k >= ROW for k in range(1, REACH)]
    wanted = jnp.concatenate(
        [offsets[0] == 0] + [o | (t[0] == k) for k, (o, t) in enumerate(zip(outside, tags), 1)]
    ).astype(jnp.int32)
    q_all = jnp.stack([flat_q] + [jnp.where(o, f, n) for o, f, n in zip(outside, far, near)])
    q_all, wanted, biases = lax.optimization_barrier((q_all, wanted, biases))

    state = flash_call(wanted, biases[0], q_all, [chunk[j] for j in ORDER[0]], None, (0, slots), caps)
    state, later = lax.optimization_barrier((state, (queries, new_cache, far_offsets, offsets)))
    own = own_call(*later[:2])
    asked = later[2][0]
    code = jnp.where(place == 2, 3, jnp.where(asked == 3, 0, asked))
    pick = jnp.broadcast_to(jnp.repeat(code, QROWS)[:, None], (last_row, HD))
    source = jnp.where(later[3][0] <= place, later[3][0], REACH)
    state, own, pick, source = lax.optimization_barrier((state, own, pick, source))
    state = flash_call(wanted, biases[1], q_all, [chunk[j] for j in ORDER[1]], state, (0, slots), caps)
    final = partial(flash_call, wanted, biases[2], q_all, [chunk[j] for j in ORDER[2]], state)
    message = [None, *final((caps, slots - caps), caps, True)]

    gathered = [
        in_row(message[1], [(7, 5)]),
        in_row(message[2], [(6, 5), (7, 6)]),
        in_row(message[3], [(7, 2)]),
    ]
    back = [in_row(message[k], [(i, i + k) for i in range(ROW - k)]) for k in range(1, REACH)]
    pick = pick[:, :1]
    passed = jnp.where(
        pick == 1,
        gathered[0],
        jnp.where(pick == 2, gathered[1], jnp.where(pick == 3, gathered[2], message[3])),
    )
    crossed = cross_row(passed, [(5, 0), (6, 1), (2, 2)], 1)
    (message[0],) = final((0, caps), caps, True)
    return merge_call(source, [message[0], *back, crossed], own, queries.shape)


def solution(mesh):
    in_specs = (
        P(None, ("group", "tensor"), None),
        P("group", None, "tensor"),
        P(None, "group", None, "tensor"),
        P("group", None),
        P("group"),
        P("group", None),
    )
    out_specs = P("group", None, "tensor")

    return jax.shard_map(shards, mesh=mesh, in_specs=in_specs, out_specs=out_specs, check_vma=False)
```

```python
from functools import partial

import jax
import jax.numpy as jnp
from jax import lax
from jax.experimental import pallas as pl
from jax.experimental.pallas import tpu as pltpu
from jax.sharding import PartitionSpec as P


HD = 128
BLOCK = 128
STEPS = 4
REACH = 4
ROW = 8
PART = 4
HEADS = 8
QROWS = 64
MSG = HEADS * HD + 128
MASKED = -1e30
ORDER = ((0, 1, 2, 3, 4), (5, 6), (7,))
SCALE2 = 1.4426950408889634 * HD ** (-0.5)


def head_rows(q):
    return jnp.concatenate([q[:, h * HD:(h + 1) * HD] for h in range(HEADS)], axis=0)


def scores_of(q, k):
    return lax.dot_general(q, k, (((1,), (1,)), ((), ())), preferred_element_type=jnp.float32) * SCALE2


def split3(x):
    hi = x.astype(jnp.bfloat16).astype(jnp.float32)
    rest = x - hi
    mid = rest.astype(jnp.bfloat16).astype(jnp.float32)
    return hi, mid, rest - mid


def flash_kernel(n_chunks, lo, first, outs_of, wanted_ref, bias_ref, q_ref, *refs):
    k_all, v_wide = refs[-2:]
    kv_refs = refs[:n_chunks]
    refs = refs[n_chunks:-2]
    if first:
        outs = refs
    else:
        acc_in, top_in = refs[:2]
        outs = refs[2:]
    tokens = kv_refs[0].shape[1]
    step = pl.program_id(0)

    @pl.when(step == 0)
    def _():
        for m in range(n_chunks):
            rows = slice(m * tokens, (m + 1) * tokens)
            k_all[rows, :] = kv_refs[m][0]
            v_wide[rows, :HD] = kv_refs[m][1]
        v_wide[:, HD:] = jnp.ones((n_chunks * tokens, HD), jnp.bfloat16)

    @pl.when(wanted_ref[lo + step] == 1)
    def _():
        lane = lax.broadcasted_iota(jnp.int32, (1, HD), 1)
        count = PART * QROWS
        parts = []
        stats = jnp.zeros((QROWS, HD), jnp.float32)
        for block in range(HEADS // PART):
            rows = slice(block * count, (block + 1) * count)
            heads = range(block * PART, (block + 1) * PART)
            q = jnp.concatenate([q_ref[0, :, h * HD:(h + 1) * HD] for h in heads], axis=0)
            s = lax.dot_general(
                q,
                k_all[...],
                (((1,), (1,)), ((), ())),
                preferred_element_type=jnp.float32,
            ) + bias_ref[...]
            top = jnp.broadcast_to(jnp.max(s, axis=1, keepdims=True), (count, HD))
            if not first:
                old = top_in[0, rows]
                top = jnp.maximum(old, top)
            p = jnp.exp2((s - top[:, 0:1]) * SCALE2).astype(jnp.bfloat16)
            acc = jnp.dot(p, v_wide[...], preferred_element_type=jnp.float32)
            if not first:
                alpha = jnp.exp2((old - top) * SCALE2)
                acc = acc + acc_in[0, rows] * jnp.concatenate([alpha, alpha], axis=1)
            if outs_of is None:
                outs[0][0, rows] = acc
                outs[1][0, rows] = top
                continue
            parts.append((acc[:, :HD] / acc[:, HD:]).astype(jnp.bfloat16))
            big = split3(top * SCALE2 + jnp.log2(acc[:, HD:]))
            for index, h in enumerate(heads):
                mine = slice(index * QROWS, (index + 1) * QROWS)
                for c in range(3):
                    stats = jnp.where(lane == c * HEADS + h, big[c][mine], stats)
        if outs_of is None:
            return
        for index, msg in enumerate(outs):
            for slot in range(outs_of):

                @pl.when(step == index * outs_of + slot)
                def _():
                    there = slice(slot * QROWS, (slot + 1) * QROWS)
                    for h in range(HEADS):
                        mine = slice(h % PART * QROWS, (h % PART + 1) * QROWS)
                        msg[there, h * HD:(h + 1) * HD] = parts[h // PART][mine]
                    msg[there, HEADS * HD:] = stats.astype(jnp.bfloat16)


def flash_call(wanted, bias, q_all, chunks, state, slots, caps, last=False):
    first = state is None
    lo, count = slots
    rows = HEADS * QROWS
    n = len(chunks)
    tokens = n * chunks[0].shape[1]
    at = lambda s, w: (lo + s, 0, 0)
    in_specs = [
        pl.BlockSpec(bias.shape, lambda s, w: (0, 0)),
        pl.BlockSpec((1, QROWS, HEADS * HD), lambda s, w: ((lo + s) // caps, (lo + s) % caps, 0)),
    ]
    in_specs += [pl.BlockSpec(c.shape, lambda s, w: (0, 0, 0)) for c in chunks]
    operands = [bias, q_all, *chunks]
    state_specs = [pl.BlockSpec((1, rows, 2 * HD), at), pl.BlockSpec((1, rows, HD), at)]
    if not first:
        in_specs += state_specs
        operands += list(state)
    if not last:
        out_specs = state_specs
        shapes = [(count, rows, 2 * HD), (count, rows, HD)]
        out_shape = [jax.ShapeDtypeStruct(s, jnp.float32) for s in shapes]
    else:
        out_specs = [pl.BlockSpec((caps * QROWS, MSG), lambda s, w: (0, 0))] * (count // caps)
        out_shape = [jax.ShapeDtypeStruct((caps * QROWS, MSG), jnp.bfloat16)] * (count // caps)
    return pl.pallas_call(
        partial(flash_kernel, n, lo, first, caps if last else None),
        grid_spec=pltpu.PrefetchScalarGridSpec(
            num_scalar_prefetch=1,
            grid=(count,),
            in_specs=in_specs,
            out_specs=out_specs,
            scratch_shapes=[
                pltpu.VMEM((tokens, HD), jnp.bfloat16),
                pltpu.VMEM((tokens, 2 * HD), jnp.bfloat16),
            ],
        ),
        out_shape=out_shape,
        compiler_params=pltpu.CompilerParams(dimension_semantics=("arbitrary",)),
        cost_estimate=pl.CostEstimate(
            flops=8 * count * rows * tokens * HD,
            transcendentals=count * rows * tokens,
            bytes_accessed=4 * tokens * HD,
        ),
        name="flash_last" if last else "flash_part",
    )(wanted, *operands)


def own_kernel(q_ref, new_ref, part_ref, stat_ref):
    lane = lax.broadcasted_iota(jnp.int32, (1, HD), 1)
    shape = (HEADS * QROWS, QROWS)
    query = lax.broadcasted_iota(jnp.int32, shape, 0) % QROWS
    token = lax.broadcasted_iota(jnp.int32, shape, 1)
    seen = (query // STEPS == token // STEPS) & (token <= query)
    for slot in range(q_ref.shape[0]):
        q = head_rows(q_ref[slot])
        s = jnp.where(seen, scores_of(q, new_ref[0, slot]), MASKED)
        m = jnp.max(s, axis=1, keepdims=True)
        p = jnp.exp2(s - m)
        l = jnp.sum(p, axis=1, keepdims=True)
        acc = jnp.dot(p.astype(jnp.bfloat16), new_ref[1, slot], preferred_element_type=jnp.float32)
        part = acc / l
        big = m + jnp.log2(l)
        stats = jnp.zeros((QROWS, HD), jnp.float32)
        for h in range(HEADS):
            rows = slice(h * QROWS, (h + 1) * QROWS)
            part_ref[slot, :, h * HD:(h + 1) * HD] = part[rows]
            stats = jnp.where(lane == h, big[rows], stats)
        stat_ref[slot] = stats


def own_call(queries, new_cache):
    slots = queries.shape[0]
    return pl.pallas_call(
        own_kernel,
        out_shape=[
            jax.ShapeDtypeStruct(queries.shape, jnp.float32),
            jax.ShapeDtypeStruct((slots, QROWS, HD), jnp.float32),
        ],
        name="own_part",
    )(queries, new_cache)


def merge_kernel(code_ref, m0, m1, m2, m3, m4, part_ref, stat_ref, out_ref, msg, sem):
    slots = out_ref.shape[0]
    for slot in range(slots):
        rows = pl.ds(slot * QROWS, QROWS)
        for index, ref in enumerate((m0, m1, m2, m3, m4)):

            @pl.when(code_ref[slot] == index)
            def _():
                pltpu.make_async_copy(ref.at[rows, :], msg.at[slot], sem.at[slot]).start()

    for slot in range(slots):
        rows = pl.ds(slot * QROWS, QROWS)
        pltpu.make_async_copy(m0.at[rows, :], msg.at[slot], sem.at[slot]).wait()
        stats = msg[slot, :, HEADS * HD:].astype(jnp.float32)
        far = stats + (
            pltpu.roll(stats, HD - HEADS, 1) + pltpu.roll(stats, HD - 2 * HEADS, 1)
        )
        near = stat_ref[slot]
        top = jnp.maximum(far, near)
        far = jnp.exp2(far - top)
        near = jnp.exp2(near - top)
        scale = 1.0 / (far + near)
        far = far * scale
        near = near * scale
        for h in range(HEADS):
            cols = slice(h * HD, (h + 1) * HD)
            out = far[:, h:h + 1] * msg[slot, :, cols].astype(jnp.float32) + (
                near[:, h:h + 1] * part_ref[slot, :, cols]
            )
            out_ref[slot, :, cols] = out.astype(out_ref.dtype)


def merge_call(code, messages, own, shape):
    vmem = pl.BlockSpec(memory_space=pltpu.VMEM)
    anywhere = pl.BlockSpec(memory_space=pltpu.HBM)
    return pl.pallas_call(
        merge_kernel,
        in_specs=[pl.BlockSpec(memory_space=pltpu.SMEM)] + [anywhere] * 5 + [vmem] * 2,
        out_specs=vmem,
        out_shape=jax.ShapeDtypeStruct(shape, jnp.bfloat16),
        scratch_shapes=[
            pltpu.VMEM((shape[0], QROWS, MSG), jnp.bfloat16),
            pltpu.SemaphoreType.DMA((shape[0],)),
        ],
        name="merge",
    )(code, *messages, *own)


def live_bias(table_row, length, member, members):
    blocks = table_row.shape[0]
    per = blocks // members
    chunk = member ^ jnp.arange(members, dtype=jnp.int32)
    physical = chunk[:, None] * per + jnp.arange(per, dtype=jnp.int32)[None, :]
    logical = jnp.sum(
        jnp.where(
            table_row[None, None, :] == physical[:, :, None],
            jnp.arange(blocks, dtype=jnp.int32)[None, None, :],
            0,
        ),
        axis=2,
    )
    position = logical[:, :, None] * BLOCK + jnp.arange(BLOCK, dtype=jnp.int32)
    bias = jnp.where(position < length, 0.0, MASKED).astype(jnp.float32)
    return bias.reshape(members, -1)


def shards(prompt_cache, queries, new_cache, offsets, lengths, block_table):
    groups = lax.axis_size("group")
    members = lax.axis_size("tensor")
    member = lax.axis_index("tensor")
    place = lax.axis_index("group") % ROW
    n_rows = groups // ROW

    def in_row(value, pairs):
        whole = [(r * ROW + a, r * ROW + b) for r in range(n_rows) for a, b in pairs]
        return lax.ppermute(value, "group", whole)

    def cross_row(value, pairs, step):
        whole = [
            (r * ROW + a, (r + step) % n_rows * ROW + b) for r in range(n_rows) for a, b in pairs
        ]
        return lax.ppermute(value, "group", whole)

    caps = queries.shape[0]
    last_row = caps * QROWS
    flat_q = queries.reshape(last_row, HEADS * HD)
    hop = in_row(flat_q, [(1, 5)])
    over = cross_row(jnp.where(place == 5, hop, flat_q), [(0, 0), (5, 5), (2, 2)], -1)
    inside = [[(i, i - k) for i in range(k, ROW)] for k in range(1, REACH)]
    tags = [in_row(offsets, inside[k - 1]) for k in range(1, REACH)]
    near = [in_row(flat_q, [(i, i - k) for i in range(k, ROW)]) for k in range(1, REACH)]

    def slab(j):
        return lax.dynamic_slice_in_dim(prompt_cache, (member ^ j) * HD, HD, 2)

    def exchanged(j):
        value = slab(j)
        return lax.ppermute(value, "tensor", [(m, m ^ j) for m in range(members)])

    chunk = {j: exchanged(j) for j in range(1, members)}
    chunk[0] = slab(0)
    far = [in_row(over, [((0, 5, 2)[i], ROW - k + i) for i in range(k)]) for k in range(1, REACH)]

    tags, far = lax.optimization_barrier((tags, far))
    live = live_bias(block_table[0], lengths[0], member, members)
    biases = [jnp.concatenate([live[j] for j in order])[None, :] for order in ORDER]
    slots = REACH * caps
    outside = [place + k >= ROW for k in range(1, REACH)]
    wanted = jnp.concatenate(
        [offsets[0] == 0] + [o | (t[0] == k) for k, (o, t) in enumerate(zip(outside, tags), 1)]
    ).astype(jnp.int32)
    q_all = jnp.stack([flat_q] + [jnp.where(o, f, n) for o, f, n in zip(outside, far, near)])
    q_all, wanted, biases = lax.optimization_barrier((q_all, wanted, biases))

    state = flash_call(wanted, biases[0], q_all, [chunk[j] for j in ORDER[0]], None, (0, slots), caps)
    state, mine, told = lax.optimization_barrier((state, (queries, new_cache), offsets))
    far_offsets = cross_row(told, [(0, 5), (1, 6)], -1)
    own = own_call(*mine)
    state, own = lax.optimization_barrier((state, own))
    state = flash_call(wanted, biases[1], q_all, [chunk[j] for j in ORDER[1]], state, (0, slots), caps)
    state, own_offsets, far_offsets = lax.optimization_barrier((state, offsets[0], far_offsets[0]))
    code = jnp.where(place == 2, 3, jnp.where(far_offsets == 3, 0, far_offsets))
    pick = jnp.broadcast_to(jnp.repeat(code, QROWS)[:, None], (last_row, HD))
    source = jnp.where(own_offsets <= place, own_offsets, REACH)
    state, pick, source = lax.optimization_barrier((state, pick, source))
    final = partial(flash_call, wanted, biases[2], q_all, [chunk[j] for j in ORDER[2]], state)
    message = [None, *final((caps, slots - caps), caps, True)]

    gathered = [
        in_row(message[1], [(7, 5)]),
        in_row(message[2], [(6, 5), (7, 6)]),
        in_row(message[3], [(7, 2)]),
    ]
    back = [in_row(message[k], [(i, i + k) for i in range(ROW - k)]) for k in range(1, REACH)]
    pick = pick[:, :1]
    passed = jnp.where(
        pick == 1,
        gathered[0],
        jnp.where(pick == 2, gathered[1], jnp.where(pick == 3, gathered[2], message[3])),
    )
    crossed = cross_row(passed, [(5, 0), (6, 1), (2, 2)], 1)
    (message[0],) = final((0, caps), caps, True)
    return merge_call(source, [message[0], *back, crossed], own, queries.shape)


def solution(mesh):
    in_specs = (
        P(None, ("group", "tensor"), None),
        P("group", None, "tensor"),
        P(None, "group", None, "tensor"),
        P("group", None),
        P("group"),
        P("group", None),
    )
    out_specs = P("group", None, "tensor")

    return jax.shard_map(shards, mesh=mesh, in_specs=in_specs, out_specs=out_specs, check_vma=False)
```

```python
from functools import partial

import jax
import jax.numpy as jnp
from jax import lax
from jax.experimental import pallas as pl
from jax.experimental.pallas import tpu as pltpu
from jax.sharding import PartitionSpec as P


HD = 128
BLOCK = 128
STEPS = 4
REACH = 4
ROW = 8
TAG = 16
PART = 4
HEADS = 8
QROWS = 64
MSG = HEADS * HD + 128
MASKED = -1e30
ORDER = ((0, 1, 2, 3, 4, 5), (6, 7))
SCALE2 = 1.4426950408889634 * HD ** (-0.5)


def head_rows(q):
    return jnp.concatenate([q[:, h * HD:(h + 1) * HD] for h in range(HEADS)], axis=0)


def scores_of(q, k):
    return lax.dot_general(q, k, (((1,), (1,)), ((), ())), preferred_element_type=jnp.float32) * SCALE2


def split3(x):
    hi = x.astype(jnp.bfloat16).astype(jnp.float32)
    rest = x - hi
    mid = rest.astype(jnp.bfloat16).astype(jnp.float32)
    return hi, mid, rest - mid


def flash_kernel(n_chunks, lo, first, outs_of, wanted_ref, bias_ref, q_ref, *refs):
    k_all, v_wide = refs[-2:]
    kv_refs = refs[:n_chunks]
    refs = refs[n_chunks:-2]
    if first:
        outs = refs
    else:
        acc_in, top_in = refs[:2]
        outs = refs[2:]
    tokens = kv_refs[0].shape[1]
    step = pl.program_id(0)

    @pl.when(step == 0)
    def _():
        for m in range(n_chunks):
            rows = slice(m * tokens, (m + 1) * tokens)
            k_all[rows, :] = kv_refs[m][0]
            v_wide[rows, :HD] = kv_refs[m][1]
        v_wide[:, HD:] = jnp.ones((n_chunks * tokens, HD), jnp.bfloat16)

    @pl.when(wanted_ref[lo + step] == 1)
    def _():
        lane = lax.broadcasted_iota(jnp.int32, (1, HD), 1)
        count = PART * QROWS
        parts = []
        stats = jnp.zeros((QROWS, HD), jnp.float32)
        for block in range(HEADS // PART):
            rows = slice(block * count, (block + 1) * count)
            heads = range(block * PART, (block + 1) * PART)
            q = jnp.concatenate([q_ref[0, :, h * HD:(h + 1) * HD] for h in heads], axis=0)
            s = lax.dot_general(
                q,
                k_all[...],
                (((1,), (1,)), ((), ())),
                preferred_element_type=jnp.float32,
            ) + bias_ref[...]
            top = jnp.broadcast_to(jnp.max(s, axis=1, keepdims=True), (count, HD))
            if not first:
                old = top_in[0, rows]
                top = jnp.maximum(old, top)
            p = jnp.exp2((s - top[:, 0:1]) * SCALE2).astype(jnp.bfloat16)
            acc = jnp.dot(p, v_wide[...], preferred_element_type=jnp.float32)
            if not first:
                alpha = jnp.exp2((old - top) * SCALE2)
                acc = acc + acc_in[0, rows] * jnp.concatenate([alpha, alpha], axis=1)
            if outs_of is None:
                outs[0][0, rows] = acc
                outs[1][0, rows] = top
                continue
            parts.append((acc[:, :HD] / acc[:, HD:]).astype(jnp.bfloat16))
            big = split3(top * SCALE2 + jnp.log2(acc[:, HD:]))
            for index, h in enumerate(heads):
                mine = slice(index * QROWS, (index + 1) * QROWS)
                for c in range(3):
                    stats = jnp.where(lane == c * HEADS + h, big[c][mine], stats)
        if outs_of is None:
            return
        for index, msg in enumerate(outs):
            for slot in range(outs_of):

                @pl.when(step == index * outs_of + slot)
                def _():
                    there = slice(slot * QROWS, (slot + 1) * QROWS)
                    for h in range(HEADS):
                        mine = slice(h % PART * QROWS, (h % PART + 1) * QROWS)
                        msg[there, h * HD:(h + 1) * HD] = parts[h // PART][mine]
                    msg[there, HEADS * HD:] = stats.astype(jnp.bfloat16)


def flash_call(wanted, bias, q_all, chunks, state, slots, caps, last=False):
    first = state is None
    lo, count = slots
    rows = HEADS * QROWS
    n = len(chunks)
    tokens = n * chunks[0].shape[1]
    at = lambda s, w: (lo + s, 0, 0)
    in_specs = [
        pl.BlockSpec(bias.shape, lambda s, w: (0, 0)),
        pl.BlockSpec((1, QROWS, HEADS * HD), lambda s, w: ((lo + s) // caps, (lo + s) % caps, 0)),
    ]
    in_specs += [pl.BlockSpec(c.shape, lambda s, w: (0, 0, 0)) for c in chunks]
    operands = [bias, q_all, *chunks]
    state_specs = [pl.BlockSpec((1, rows, 2 * HD), at), pl.BlockSpec((1, rows, HD), at)]
    if not first:
        in_specs += state_specs
        operands += list(state)
    if not last:
        out_specs = state_specs
        shapes = [(count, rows, 2 * HD), (count, rows, HD)]
        out_shape = [jax.ShapeDtypeStruct(s, jnp.float32) for s in shapes]
    else:
        out_specs = [pl.BlockSpec((caps * QROWS, MSG), lambda s, w: (0, 0))] * (count // caps)
        out_shape = [jax.ShapeDtypeStruct((caps * QROWS, MSG), jnp.bfloat16)] * (count // caps)
    return pl.pallas_call(
        partial(flash_kernel, n, lo, first, caps if last else None),
        grid_spec=pltpu.PrefetchScalarGridSpec(
            num_scalar_prefetch=1,
            grid=(count,),
            in_specs=in_specs,
            out_specs=out_specs,
            scratch_shapes=[
                pltpu.VMEM((tokens, HD), jnp.bfloat16),
                pltpu.VMEM((tokens, 2 * HD), jnp.bfloat16),
            ],
        ),
        out_shape=out_shape,
        compiler_params=pltpu.CompilerParams(dimension_semantics=("arbitrary",)),
        cost_estimate=pl.CostEstimate(
            flops=8 * count * rows * tokens * HD,
            transcendentals=count * rows * tokens,
            bytes_accessed=4 * tokens * HD,
        ),
        name="flash_last" if last else "flash_part",
    )(wanted, *operands)


def own_kernel(q_ref, new_ref, part_ref, stat_ref):
    lane = lax.broadcasted_iota(jnp.int32, (1, HD), 1)
    shape = (HEADS * QROWS, QROWS)
    query = lax.broadcasted_iota(jnp.int32, shape, 0) % QROWS
    token = lax.broadcasted_iota(jnp.int32, shape, 1)
    seen = (query // STEPS == token // STEPS) & (token <= query)
    for slot in range(q_ref.shape[0]):
        q = head_rows(q_ref[slot])
        s = jnp.where(seen, scores_of(q, new_ref[0, slot]), MASKED)
        m = jnp.max(s, axis=1, keepdims=True)
        p = jnp.exp2(s - m)
        l = jnp.sum(p, axis=1, keepdims=True)
        acc = jnp.dot(p.astype(jnp.bfloat16), new_ref[1, slot], preferred_element_type=jnp.float32)
        part = acc / l
        big = m + jnp.log2(l)
        stats = jnp.zeros((QROWS, HD), jnp.float32)
        for h in range(HEADS):
            rows = slice(h * QROWS, (h + 1) * QROWS)
            part_ref[slot, :, h * HD:(h + 1) * HD] = part[rows]
            stats = jnp.where(lane == h, big[rows], stats)
        stat_ref[slot] = stats


def own_call(queries, new_cache):
    slots = queries.shape[0]
    return pl.pallas_call(
        own_kernel,
        out_shape=[
            jax.ShapeDtypeStruct(queries.shape, jnp.float32),
            jax.ShapeDtypeStruct((slots, QROWS, HD), jnp.float32),
        ],
        name="own_part",
    )(queries, new_cache)


def merge_kernel(code_ref, m0, m1, m2, m3, m4, part_ref, stat_ref, out_ref, msg, sem):
    slots = out_ref.shape[0]
    for slot in range(slots):
        rows = pl.ds(slot * QROWS, QROWS)
        for index, ref in enumerate((m0, m1, m2, m3, m4)):

            @pl.when(code_ref[slot] == index)
            def _():
                pltpu.make_async_copy(ref.at[rows, :], msg.at[slot], sem.at[slot]).start()

    for slot in range(slots):
        rows = pl.ds(slot * QROWS, QROWS)
        pltpu.make_async_copy(m0.at[rows, :], msg.at[slot], sem.at[slot]).wait()
        stats = msg[slot, :, HEADS * HD:].astype(jnp.float32)
        far = stats + (
            pltpu.roll(stats, HD - HEADS, 1) + pltpu.roll(stats, HD - 2 * HEADS, 1)
        )
        near = stat_ref[slot]
        top = jnp.maximum(far, near)
        far = jnp.exp2(far - top)
        near = jnp.exp2(near - top)
        scale = 1.0 / (far + near)
        far = far * scale
        near = near * scale
        for h in range(HEADS):
            cols = slice(h * HD, (h + 1) * HD)
            out = far[:, h:h + 1] * msg[slot, :, cols].astype(jnp.float32) + (
                near[:, h:h + 1] * part_ref[slot, :, cols]
            )
            out_ref[slot, :, cols] = out.astype(out_ref.dtype)


def merge_call(code, messages, own, shape):
    vmem = pl.BlockSpec(memory_space=pltpu.VMEM)
    anywhere = pl.BlockSpec(memory_space=pltpu.HBM)
    return pl.pallas_call(
        merge_kernel,
        in_specs=[pl.BlockSpec(memory_space=pltpu.SMEM)] + [anywhere] * 5 + [vmem] * 2,
        out_specs=vmem,
        out_shape=jax.ShapeDtypeStruct(shape, jnp.bfloat16),
        scratch_shapes=[
            pltpu.VMEM((shape[0], QROWS, MSG), jnp.bfloat16),
            pltpu.SemaphoreType.DMA((shape[0],)),
        ],
        name="merge",
    )(code, *messages, *own)


def live_bias(table_row, length, member, members):
    blocks = table_row.shape[0]
    per = blocks // members
    chunk = member ^ jnp.arange(members, dtype=jnp.int32)
    physical = chunk[:, None] * per + jnp.arange(per, dtype=jnp.int32)[None, :]
    logical = jnp.sum(
        jnp.where(
            table_row[None, None, :] == physical[:, :, None],
            jnp.arange(blocks, dtype=jnp.int32)[None, None, :],
            0,
        ),
        axis=2,
    )
    position = logical[:, :, None] * BLOCK + jnp.arange(BLOCK, dtype=jnp.int32)
    bias = jnp.where(position < length, 0.0, MASKED).astype(jnp.float32)
    return bias.reshape(members, -1)


def shards(prompt_cache, queries, new_cache, offsets, lengths, block_table):
    groups = lax.axis_size("group")
    members = lax.axis_size("tensor")
    member = lax.axis_index("tensor")
    place = lax.axis_index("group") % ROW
    n_rows = groups // ROW

    def in_row(value, pairs):
        whole = [(r * ROW + a, r * ROW + b) for r in range(n_rows) for a, b in pairs]
        return lax.ppermute(value, "group", whole)

    def cross_row(value, pairs, step):
        whole = [
            (r * ROW + a, (r + step) % n_rows * ROW + b) for r in range(n_rows) for a, b in pairs
        ]
        return lax.ppermute(value, "group", whole)

    caps = queries.shape[0]
    last_row = caps * QROWS
    marks = jnp.repeat(offsets[0].astype(jnp.bfloat16), TAG // caps)
    tagged = jnp.concatenate(
        [
            queries.reshape(last_row, HEADS * HD),
            jnp.broadcast_to(marks[:, None], (TAG, HEADS * HD)),
        ],
        axis=0,
    )
    hop = in_row(tagged, [(1, 5)])
    over = cross_row(jnp.where(place == 5, hop, tagged), [(0, 0), (5, 5), (2, 2)], -1)
    near = [in_row(tagged, [(i, i - k) for i in range(k, ROW)]) for k in range(1, REACH)]

    def slab(j):
        return lax.dynamic_slice_in_dim(prompt_cache, (member ^ j) * HD, HD, 2)

    def exchanged(j):
        value = slab(j)
        return lax.ppermute(value, "tensor", [(m, m ^ j) for m in range(members)])

    chunk = {j: exchanged(j) for j in range(1, members)}
    chunk[0] = slab(0)
    far = [in_row(over, [((0, 5, 2)[i], ROW - k + i) for i in range(k)]) for k in range(1, REACH)]

    live = live_bias(block_table[0], lengths[0], member, members)
    biases = [jnp.concatenate([live[j] for j in order])[None, :] for order in ORDER]
    slots = REACH * caps
    q_all = jnp.stack(
        [tagged]
        + [jnp.where(place + k >= ROW, far[k - 1], near[k - 1]) for k in range(1, REACH)]
    )
    asked = q_all[:, last_row::TAG // caps, 0].astype(jnp.int32)
    wanted = (asked == jnp.arange(REACH, dtype=jnp.int32)[:, None]).astype(jnp.int32).reshape(-1)
    q_all, wanted, biases = lax.optimization_barrier((q_all, wanted, biases))

    state = flash_call(wanted, biases[0], q_all, [chunk[j] for j in ORDER[0]], None, (0, slots), caps)
    state, mine, asked, own_offsets = lax.optimization_barrier(
        (state, (queries, new_cache), asked[3], offsets[0])
    )
    own = own_call(*mine)
    code = jnp.where(place == 2, 3, jnp.where(asked == 3, 0, asked))
    pick = jnp.broadcast_to(jnp.repeat(code, QROWS)[:, None], (last_row, HD))
    source = jnp.where(own_offsets <= place, own_offsets, REACH)
    state, own, pick, source = lax.optimization_barrier((state, own, pick, source))
    final = partial(flash_call, wanted, biases[1], q_all, [chunk[j] for j in ORDER[1]], state)
    message = [None, *final((caps, slots - caps), caps, True)]

    gathered = [
        in_row(message[1], [(7, 5)]),
        in_row(message[2], [(6, 5), (7, 6)]),
        in_row(message[3], [(7, 2)]),
    ]
    back = [in_row(message[k], [(i, i + k) for i in range(ROW - k)]) for k in range(1, REACH)]
    pick = pick[:, :1]
    passed = jnp.where(
        pick == 1,
        gathered[0],
        jnp.where(pick == 2, gathered[1], jnp.where(pick == 3, gathered[2], message[3])),
    )
    crossed = cross_row(passed, [(5, 0), (6, 1), (2, 2)], 1)
    (message[0],) = final((0, caps), caps, True)
    return merge_call(source, [message[0], *back, crossed], own, queries.shape)


def solution(mesh):
    in_specs = (
        P(None, ("group", "tensor"), None),
        P("group", None, "tensor"),
        P(None, "group", None, "tensor"),
        P("group", None),
        P("group"),
        P("group", None),
    )
    out_specs = P("group", None, "tensor")

    return jax.shard_map(shards, mesh=mesh, in_specs=in_specs, out_specs=out_specs, check_vma=False)
```

```python
from functools import partial

import jax
import jax.numpy as jnp
from jax import lax
from jax.experimental import pallas as pl
from jax.experimental.pallas import tpu as pltpu
from jax.sharding import PartitionSpec as P


HD = 128
BLOCK = 128
STEPS = 4
REACH = 4
ROW = 8
TAG = 16
PART = 4
HEADS = 8
QROWS = 64
MSG = HEADS * HD + 128
MASKED = -1e30
ORDER = ((0, 1, 4, 2), (5, 3, 6), (7,))
SCALE2 = 1.4426950408889634 * HD ** (-0.5)


def head_rows(q):
    return jnp.concatenate([q[:, h * HD:(h + 1) * HD] for h in range(HEADS)], axis=0)


def scores_of(q, k):
    return lax.dot_general(q, k, (((1,), (1,)), ((), ())), preferred_element_type=jnp.float32) * SCALE2


def split3(x):
    hi = x.astype(jnp.bfloat16).astype(jnp.float32)
    rest = x - hi
    mid = rest.astype(jnp.bfloat16).astype(jnp.float32)
    return hi, mid, rest - mid


def flash_kernel(n_chunks, lo, first, outs_of, wanted_ref, bias_ref, q_ref, *refs):
    k_all, v_wide = refs[-2:]
    kv_refs = refs[:n_chunks]
    refs = refs[n_chunks:-2]
    if first:
        outs = refs
    else:
        acc_in, top_in = refs[:2]
        outs = refs[2:]
    tokens = kv_refs[0].shape[1]
    step = pl.program_id(0)

    @pl.when(step == 0)
    def _():
        for m in range(n_chunks):
            rows = slice(m * tokens, (m + 1) * tokens)
            k_all[rows, :] = kv_refs[m][0]
            v_wide[rows, :HD] = kv_refs[m][1]
        v_wide[:, HD:] = jnp.ones((n_chunks * tokens, HD), jnp.bfloat16)

    @pl.when(wanted_ref[lo + step] == 1)
    def _():
        lane = lax.broadcasted_iota(jnp.int32, (1, HD), 1)
        count = PART * QROWS
        parts = []
        stats = jnp.zeros((QROWS, HD), jnp.float32)
        for block in range(HEADS // PART):
            rows = slice(block * count, (block + 1) * count)
            heads = range(block * PART, (block + 1) * PART)
            q = jnp.concatenate([q_ref[0, :, h * HD:(h + 1) * HD] for h in heads], axis=0)
            s = lax.dot_general(
                q,
                k_all[...],
                (((1,), (1,)), ((), ())),
                preferred_element_type=jnp.float32,
            ) + bias_ref[...]
            top = jnp.broadcast_to(jnp.max(s, axis=1, keepdims=True), (count, HD))
            if not first:
                old = top_in[0, rows]
                top = jnp.maximum(old, top)
            p = jnp.exp2((s - top[:, 0:1]) * SCALE2).astype(jnp.bfloat16)
            acc = jnp.dot(p, v_wide[...], preferred_element_type=jnp.float32)
            if not first:
                alpha = jnp.exp2((old - top) * SCALE2)
                acc = acc + acc_in[0, rows] * jnp.concatenate([alpha, alpha], axis=1)
            if outs_of is None:
                outs[0][0, rows] = acc
                outs[1][0, rows] = top
                continue
            parts.append((acc[:, :HD] / acc[:, HD:]).astype(jnp.bfloat16))
            big = split3(top * SCALE2 + jnp.log2(acc[:, HD:]))
            for index, h in enumerate(heads):
                mine = slice(index * QROWS, (index + 1) * QROWS)
                for c in range(3):
                    stats = jnp.where(lane == c * HEADS + h, big[c][mine], stats)
        if outs_of is None:
            return
        for index, msg in enumerate(outs):
            for slot in range(outs_of):

                @pl.when(step == index * outs_of + slot)
                def _():
                    there = slice(slot * QROWS, (slot + 1) * QROWS)
                    for h in range(HEADS):
                        mine = slice(h % PART * QROWS, (h % PART + 1) * QROWS)
                        msg[there, h * HD:(h + 1) * HD] = parts[h // PART][mine]
                    msg[there, HEADS * HD:] = stats.astype(jnp.bfloat16)


def flash_call(wanted, bias, q_all, chunks, state, slots, caps, last=False):
    first = state is None
    lo, count = slots
    rows = HEADS * QROWS
    n = len(chunks)
    tokens = n * chunks[0].shape[1]
    at = lambda s, w: (lo + s, 0, 0)
    in_specs = [
        pl.BlockSpec(bias.shape, lambda s, w: (0, 0)),
        pl.BlockSpec((1, QROWS, HEADS * HD), lambda s, w: ((lo + s) // caps, (lo + s) % caps, 0)),
    ]
    in_specs += [pl.BlockSpec(c.shape, lambda s, w: (0, 0, 0)) for c in chunks]
    operands = [bias, q_all, *chunks]
    state_specs = [pl.BlockSpec((1, rows, 2 * HD), at), pl.BlockSpec((1, rows, HD), at)]
    if not first:
        in_specs += state_specs
        operands += list(state)
    if not last:
        out_specs = state_specs
        shapes = [(count, rows, 2 * HD), (count, rows, HD)]
        out_shape = [jax.ShapeDtypeStruct(s, jnp.float32) for s in shapes]
    else:
        out_specs = [pl.BlockSpec((caps * QROWS, MSG), lambda s, w: (0, 0))] * (count // caps)
        out_shape = [jax.ShapeDtypeStruct((caps * QROWS, MSG), jnp.bfloat16)] * (count // caps)
    return pl.pallas_call(
        partial(flash_kernel, n, lo, first, caps if last else None),
        grid_spec=pltpu.PrefetchScalarGridSpec(
            num_scalar_prefetch=1,
            grid=(count,),
            in_specs=in_specs,
            out_specs=out_specs,
            scratch_shapes=[
                pltpu.VMEM((tokens, HD), jnp.bfloat16),
                pltpu.VMEM((tokens, 2 * HD), jnp.bfloat16),
            ],
        ),
        out_shape=out_shape,
        compiler_params=pltpu.CompilerParams(dimension_semantics=("arbitrary",)),
        cost_estimate=pl.CostEstimate(
            flops=8 * count * rows * tokens * HD,
            transcendentals=count * rows * tokens,
            bytes_accessed=4 * tokens * HD,
        ),
        name="flash_last" if last else "flash_part",
    )(wanted, *operands)


def own_kernel(q_ref, new_ref, part_ref, stat_ref):
    lane = lax.broadcasted_iota(jnp.int32, (1, HD), 1)
    shape = (HEADS * QROWS, QROWS)
    query = lax.broadcasted_iota(jnp.int32, shape, 0) % QROWS
    token = lax.broadcasted_iota(jnp.int32, shape, 1)
    seen = (query // STEPS == token // STEPS) & (token <= query)
    for slot in range(q_ref.shape[0]):
        q = head_rows(q_ref[slot])
        s = jnp.where(seen, scores_of(q, new_ref[0, slot]), MASKED)
        m = jnp.max(s, axis=1, keepdims=True)
        p = jnp.exp2(s - m)
        l = jnp.sum(p, axis=1, keepdims=True)
        acc = jnp.dot(p.astype(jnp.bfloat16), new_ref[1, slot], preferred_element_type=jnp.float32)
        part = acc / l
        big = m + jnp.log2(l)
        stats = jnp.zeros((QROWS, HD), jnp.float32)
        for h in range(HEADS):
            rows = slice(h * QROWS, (h + 1) * QROWS)
            part_ref[slot, :, h * HD:(h + 1) * HD] = part[rows]
            stats = jnp.where(lane == h, big[rows], stats)
        stat_ref[slot] = stats


def own_call(queries, new_cache):
    slots = queries.shape[0]
    return pl.pallas_call(
        own_kernel,
        out_shape=[
            jax.ShapeDtypeStruct(queries.shape, jnp.float32),
            jax.ShapeDtypeStruct((slots, QROWS, HD), jnp.float32),
        ],
        name="own_part",
    )(queries, new_cache)


def merge_kernel(code_ref, m0, m1, m2, m3, m4, m5, part_ref, stat_ref, out_ref, msg, sem):
    slots = out_ref.shape[0]
    for slot in range(slots):
        rows = pl.ds(slot * QROWS, QROWS)
        for index, ref in enumerate((m0, m1, m2, m3, m4, m5)):

            @pl.when(code_ref[slot] == index)
            def _():
                pltpu.make_async_copy(ref.at[rows, :], msg.at[slot], sem.at[slot]).start()

    for slot in range(slots):
        rows = pl.ds(slot * QROWS, QROWS)
        pltpu.make_async_copy(m0.at[rows, :], msg.at[slot], sem.at[slot]).wait()
        stats = msg[slot, :, HEADS * HD:].astype(jnp.float32)
        far = stats + (
            pltpu.roll(stats, HD - HEADS, 1) + pltpu.roll(stats, HD - 2 * HEADS, 1)
        )
        near = stat_ref[slot]
        top = jnp.maximum(far, near)
        far = jnp.exp2(far - top)
        near = jnp.exp2(near - top)
        scale = 1.0 / (far + near)
        far = far * scale
        near = near * scale
        for h in range(HEADS):
            cols = slice(h * HD, (h + 1) * HD)
            out = far[:, h:h + 1] * msg[slot, :, cols].astype(jnp.float32) + (
                near[:, h:h + 1] * part_ref[slot, :, cols]
            )
            out_ref[slot, :, cols] = out.astype(out_ref.dtype)


def merge_call(code, messages, own, shape):
    vmem = pl.BlockSpec(memory_space=pltpu.VMEM)
    anywhere = pl.BlockSpec(memory_space=pltpu.HBM)
    return pl.pallas_call(
        merge_kernel,
        in_specs=[pl.BlockSpec(memory_space=pltpu.SMEM)] + [anywhere] * 6 + [vmem] * 2,
        out_specs=vmem,
        out_shape=jax.ShapeDtypeStruct(shape, jnp.bfloat16),
        scratch_shapes=[
            pltpu.VMEM((shape[0], QROWS, MSG), jnp.bfloat16),
            pltpu.SemaphoreType.DMA((shape[0],)),
        ],
        name="merge",
    )(code, *messages, *own)


def live_bias(table_row, length, member, members):
    blocks = table_row.shape[0]
    per = blocks // members
    chunk = member ^ jnp.arange(members, dtype=jnp.int32)
    physical = chunk[:, None] * per + jnp.arange(per, dtype=jnp.int32)[None, :]
    logical = jnp.sum(
        jnp.where(
            table_row[None, None, :] == physical[:, :, None],
            jnp.arange(blocks, dtype=jnp.int32)[None, None, :],
            0,
        ),
        axis=2,
    )
    position = logical[:, :, None] * BLOCK + jnp.arange(BLOCK, dtype=jnp.int32)
    bias = jnp.where(position < length, 0.0, MASKED).astype(jnp.float32)
    return bias.reshape(members, -1)


def shards(prompt_cache, queries, new_cache, offsets, lengths, block_table):
    groups = lax.axis_size("group")
    members = lax.axis_size("tensor")
    member = lax.axis_index("tensor")
    place = lax.axis_index("group") % ROW
    n_rows = groups // ROW

    def in_row(value, pairs):
        whole = [(r * ROW + a, r * ROW + b) for r in range(n_rows) for a, b in pairs]
        return lax.ppermute(value, "group", whole)

    def cross_row(value, pairs, step):
        whole = [
            (r * ROW + a, (r + step) % n_rows * ROW + b) for r in range(n_rows) for a, b in pairs
        ]
        return lax.ppermute(value, "group", whole)

    caps = queries.shape[0]
    last_row = caps * QROWS
    marks = jnp.repeat(offsets[0].astype(jnp.bfloat16), TAG // caps)
    tagged = jnp.concatenate(
        [
            queries.reshape(last_row, HEADS * HD),
            jnp.broadcast_to(marks[:, None], (TAG, HEADS * HD)),
        ],
        axis=0,
    )
    hop = in_row(tagged, [(1, 5)])
    over = cross_row(jnp.where(place == 5, hop, tagged), [(0, 0), (5, 5), (2, 2)], -1)
    near = [in_row(tagged, [(i, i - k) for i in range(k, ROW)]) for k in range(1, REACH)]

    def slab(j):
        return lax.dynamic_slice_in_dim(prompt_cache, (member ^ j) * HD, HD, 2)

    def exchanged(j):
        value = slab(j)
        return lax.ppermute(value, "tensor", [(m, m ^ j) for m in range(members)])

    chunk = {j: exchanged(j) for j in range(1, members)}
    chunk[0] = slab(0)
    far = [in_row(over, [((0, 5, 2)[i], ROW - k + i) for i in range(k)]) for k in range(1, REACH)]

    live = live_bias(block_table[0], lengths[0], member, members)
    biases = [jnp.concatenate([live[j] for j in order])[None, :] for order in ORDER]
    slots = REACH * caps
    q_all = jnp.stack(
        [tagged]
        + [jnp.where(place + k >= ROW, far[k - 1], near[k - 1]) for k in range(1, REACH)]
    )
    asked = q_all[:, last_row::TAG // caps, 0].astype(jnp.int32)
    wanted = (asked == jnp.arange(REACH, dtype=jnp.int32)[:, None]).astype(jnp.int32).reshape(-1)
    q_all, wanted, biases = lax.optimization_barrier((q_all, wanted, biases))

    state = flash_call(wanted, biases[0], q_all, [chunk[j] for j in ORDER[0]], None, (0, slots), caps)
    state, mine, asked, own_offsets = lax.optimization_barrier(
        (state, (queries, new_cache), asked[3], offsets[0])
    )
    own = own_call(*mine)
    pick = jnp.broadcast_to(jnp.repeat(asked, QROWS)[:, None], (last_row, HD))
    source = jnp.where(own_offsets <= place, own_offsets, jnp.where(place == 2, REACH + 1, REACH))
    state, own, pick, source = lax.optimization_barrier((state, own, pick, source))
    state = flash_call(wanted, biases[1], q_all, [chunk[j] for j in ORDER[1]], state, (0, slots), caps)
    final = partial(flash_call, wanted, biases[2], q_all, [chunk[j] for j in ORDER[2]], state)
    message = [None, *final((caps, slots - caps), caps, True)]

    gathered = [in_row(message[1], [(7, 5)]), in_row(message[2], [(6, 5), (7, 6)])]
    direct = cross_row(message[3], [(7, 2)], 1)
    back = [in_row(message[k], [(i, i + k) for i in range(ROW - k)]) for k in range(1, REACH)]
    pick = pick[:, :1]
    passed = jnp.where(pick == 1, gathered[0], jnp.where(pick == 2, gathered[1], message[3]))
    crossed = cross_row(passed, [(5, 0), (6, 1)], 1)
    (message[0],) = final((0, caps), caps, True)
    return merge_call(source, [message[0], *back, crossed, direct], own, queries.shape)


def solution(mesh):
    in_specs = (
        P(None, ("group", "tensor"), None),
        P("group", None, "tensor"),
        P(None, "group", None, "tensor"),
        P("group", None),
        P("group"),
        P("group", None),
    )
    out_specs = P("group", None, "tensor")

    return jax.shard_map(shards, mesh=mesh, in_specs=in_specs, out_specs=out_specs, check_vma=False)
```
